32 devices in a mesh: pb: 4 (over y, x), wa: 8 (over z, core).
Axes of the slice: x: 2, y: 2, z: 4, core: 2. Of those that a mesh axis runs over, the one named last changes fastest.
Arguments:
- quartets: int32 [1024, 4, 128], P(('pb', 'wa')), may hold values from -1 to 49151, as said below
- counts: int32 [32], P(('pb', 'wa')), may hold values from 1 to 32, as said below
- eig: bfloat16 [24, 49152], P(None, 'pb'), may hold values from -1.1953125 to 1.1953125
- freq: bfloat16 [49152], P('pb'), may hold values from 0.5 to 2
- phi: bfloat16 [144, 1152], replicated, may hold values from -0.5390625 to 0.5390625
- cells: int32 [8, 9], replicated, may hold values from -2 to 2
Outputs:
- rates: float32 [49152], P(('pb', 'wa'))
The draws below stay inside these ranges and needn't reach their ends.
Inputs may be any that keep to these rules, and one draw needn't show every extreme that they name: quartets[b, 0, n] is a mode of one of the 1024 q-points of the owner group of slot b (from 0 to 12287); the other three entries are all -1 or all modes of the mesh, and then their q-points and that of the first add up as q1 + q2 = q3 + q4 on the mesh. The used slots of a device are its first counts slots; some device has exactly 32.
All inputs are finite; a program needn't handle non-finite values.
Results may differ from the reference program's by a relative error of at most 0.0023.
Values may be sent and summed in bfloat16 or wider, within the bound.
A program may use at most 64 MiB of HBM per device.

```python
import math
import jax
import jax.numpy as jnp
from jax import lax

QMESH = 16
BRANCHES = 12
CLUSTERS = 8
BLOCK = 128
BLK_DEV = 32
NQ = 4096
NMODE = 49152
Q_DEV = 1024
WORKERS = 32
SHARD_BLK = 256
NBLK = 1024


def mesh_point(across, along, upward):
    return (across * QMESH + along) * QMESH + upward


def draw_quartets(key, part):
    local_q = jax.random.randint(jax.random.fold_in(key, 1), (NBLK, 1), 0, Q_DEV)
    owner = (jnp.arange(NBLK, dtype=jnp.int32) // SHARD_BLK)[:, None]
    first_q = owner * Q_DEV + local_q
    second_q = jax.random.randint(jax.random.fold_in(key, 2), (NBLK, BLOCK), 0, NQ)
    third_q = jax.random.randint(jax.random.fold_in(key, 3), (NBLK, BLOCK), 0, NQ)
    square = QMESH * QMESH
    fourth_q = mesh_point(jnp.remainder(first_q // square + second_q // square - third_q // square, QMESH), jnp.remainder(first_q // QMESH % QMESH + second_q // QMESH % QMESH - third_q // QMESH % QMESH, QMESH), jnp.remainder(first_q % QMESH + second_q % QMESH - third_q % QMESH, QMESH))
    branch_draw = jax.random.randint(jax.random.fold_in(key, 4), (4, NBLK, BLOCK), 0, BRANCHES)
    pad_length = jax.random.randint(jax.random.fold_in(key, 5), (NBLK, 1), 0, BLOCK // 2 + 1)
    padded = jnp.arange(BLOCK, dtype=jnp.int32)[None, :] >= BLOCK - pad_length
    first_mode = local_q * BRANCHES + branch_draw[0]
    second_mode = jnp.where(padded, -1, second_q * BRANCHES + branch_draw[1])
    third_mode = jnp.where(padded, -1, third_q * BRANCHES + branch_draw[2])
    fourth_mode = jnp.where(padded, -1, fourth_q * BRANCHES + branch_draw[3])
    return jnp.stack([first_mode, second_mode, third_mode, fourth_mode], axis=1).astype(jnp.int32)


def draw_counts(key, part):
    first_draw = jax.random.randint(jax.random.fold_in(key, 11), (WORKERS,), 1, BLK_DEV + 1)
    second_draw = jax.random.randint(jax.random.fold_in(key, 12), (WORKERS,), 1, BLK_DEV + 1)
    chosen = jax.random.randint(jax.random.fold_in(key, 13), (), 0, WORKERS)
    tally = jnp.maximum(1, first_draw * second_draw // BLK_DEV)
    tally = jnp.where(jnp.arange(WORKERS, dtype=jnp.int32) == chosen, BLK_DEV, tally)
    return tally.astype(jnp.int32)


def with_ends(values, key, low, high):
    place = [jax.random.randint(jax.random.fold_in(key, axis), (), 0, length) for axis, length in enumerate(values.shape)]
    widest = values.shape.index(max(values.shape))
    beside = place[:widest] + [(place[widest] + 1) % values.shape[widest]] + place[widest + 1:]
    return values.at[tuple(place)].set(low).at[tuple(beside)].set(high)


def steps_of(rng, extent, shards, low, largest):
    def one(position, shards_of):
        steps = jax.random.uniform(jax.random.fold_in(jax.random.fold_in(rng, 6), position), (shards_of,), jnp.float32, low / len(shards), largest / len(shards))
        return jnp.repeat(jnp.exp(steps), extent[position] // shards_of).reshape((-1,) + (1,) * (len(extent) - position - 1))

    factor_of = one(*shards[0])
    for cut in shards[1:]:
        factor_of = factor_of * one(*cut)
    return factor_of


def centred(rng, extent, spread, limit, shards=(), held_as=jnp.bfloat16):
    drawn = jax.random.normal(rng, extent, jnp.float32) * spread
    if len(shards) > 0:
        drawn = steps_of(rng, extent, shards, -0.22, 0.18) * drawn
    return jnp.clip(drawn, min=-limit, max=limit).astype(held_as)


def setup_inputs(seed: int = 0) -> dict:
    key_list = jax.random.split(jax.random.key(seed), 7)
    return {
        "quartets": draw_quartets(jax.random.fold_in(key_list[6], 71), 0),
        "counts": draw_counts(jax.random.fold_in(key_list[6], 71), 0),
        "eig": centred(key_list[2], (2 * BRANCHES, NMODE), 0.2, 1.1953125, ((1, 4),)),
        "freq": jnp.clip(jnp.exp(math.log(2.0) - 1.3862944 * jax.random.uniform(key_list[3], (NMODE,), jnp.float32) ** steps_of(key_list[3], (NMODE,), ((0, 4),), -0.2, 0.2)), 0.5, 2.0).astype(jnp.bfloat16),
        "phi": centred(key_list[4], (BRANCHES * BRANCHES, CLUSTERS * BRANCHES * BRANCHES), 0.09, 0.5390625),
        "cells": with_ends(jax.random.randint(key_list[5], (CLUSTERS, 9), -2, 3), jax.random.fold_in(key_list[5], 1), -2, 2).astype(jnp.int32),
    }


smearing = 0.5

def outer_pair(first, second, branches):
    count = first.shape[1]
    first_re = first[:branches][:, None, :]
    first_im = first[branches:][:, None, :]
    second_re = second[:branches][None, :, :]
    second_im = second[branches:][None, :, :]
    real = (first_re * second_re - first_im * second_im).reshape(branches * branches, count)
    imag = (first_re * second_im + first_im * second_re).reshape(branches * branches, count)
    return (real, imag)

def cluster_phase(other_modes, cells, branches):
    points = other_modes // branches
    coords = [points // (QMESH * QMESH), points // QMESH % QMESH, points % QMESH]
    shift = jnp.zeros((cells.shape[0], other_modes.shape[1]), jnp.int32)
    for which in range(3):
        sign = 1 if which == 0 else -1
        for axis_c in range(3):
            shift = shift + sign * cells[:, 3 * which + axis_c][:, None] * coords[axis_c][which][None, :]
    angle = jnp.remainder(shift, QMESH).astype(jnp.float32) * (2.0 * math.pi / QMESH)
    return (jnp.cos(angle), jnp.sin(angle))

def occupation(value):
    return 1.0 / (jnp.exp(value) - 1.0)

def contributions(first_modes, other_modes, other_spots, valid, first_vectors, first_freqs, vectors, frequencies, phi, cells):
    branches = vectors.shape[0] // 2
    count = first_modes.shape[0]
    clusters = cells.shape[0]
    first_vec = jnp.take(first_vectors, first_modes, axis=1).astype(jnp.float32)
    first_freq = jnp.take(first_freqs, first_modes).astype(jnp.float32)
    flat_spots = other_spots.reshape(3 * count)
    gathered = jnp.take(vectors, flat_spots, axis=1).astype(jnp.float32)
    other_freq = jnp.take(frequencies, flat_spots).astype(jnp.float32).reshape(3, count)
    second_vec = gathered[:, :count]
    third_vec = gathered[:, count:2 * count]
    fourth_vec = gathered[:, 2 * count:]
    far_re, far_im = outer_pair(third_vec, fourth_vec, branches)
    far_im = -far_im
    cosine, sine = cluster_phase(other_modes, cells, branches)
    wide_re = cosine[:, None, :] * far_re[None] - sine[:, None, :] * far_im[None]
    wide_im = cosine[:, None, :] * far_im[None] + sine[:, None, :] * far_re[None]
    wide_re = wide_re.reshape(clusters * branches * branches, count).astype(jnp.bfloat16)
    wide_im = wide_im.reshape(clusters * branches * branches, count).astype(jnp.bfloat16)
    weighted_re = jnp.dot(phi, wide_re, preferred_element_type=jnp.float32)
    weighted_im = jnp.dot(phi, wide_im, preferred_element_type=jnp.float32)
    near_re, near_im = outer_pair(first_vec, second_vec, branches)
    value_re = lax.optimization_barrier(jnp.sum(near_re * weighted_re - near_im * weighted_im, axis=0))
    value_im = lax.optimization_barrier(jnp.sum(near_re * weighted_im + near_im * weighted_re, axis=0))
    mismatch = first_freq + other_freq[0] - other_freq[1] - other_freq[2]
    delta = jnp.exp(-(mismatch / smearing) ** 2) / (smearing * math.sqrt(math.pi))
    weight = (1.0 + occupation(other_freq[0])) * occupation(other_freq[1]) * occupation(other_freq[2]) / occupation(first_freq)
    product = first_freq * other_freq[0] * other_freq[1] * other_freq[2]
    return jnp.where(valid, (value_re * value_re + value_im * value_im) * delta * weight / product, 0.0)

def reference(quartets, counts, eig, freq, phi, cells):
    total_blocks = quartets.shape[0]
    block = quartets.shape[2]
    group = math.gcd(BLK_DEV, 16)
    index = jnp.arange(total_blocks, dtype=jnp.int32)
    used = index % BLK_DEV < jnp.take(counts, index // BLK_DEV)
    rank = (jnp.cumsum(used.astype(jnp.int32)) - 1).astype(jnp.int32)
    target = jnp.where(used, rank, total_blocks).astype(jnp.int32)
    order = jnp.zeros((total_blocks,), jnp.int32).at[target].set(index, mode='drop')
    total = jnp.sum(used.astype(jnp.int32)).astype(jnp.int32)
    offsets = (index // SHARD_BLK * (Q_DEV * BRANCHES)).astype(jnp.int32)
    rounds = (total + group - 1) // group

    def one_round(step, rates):
        start = (step * group).astype(jnp.int32)
        picks = lax.dynamic_slice_in_dim(order, start, group, 0)
        blocks = jnp.take(quartets, picks, axis=0)
        live = start + jnp.arange(group, dtype=jnp.int32) < total
        first_modes = (blocks[:, 0, :] + jnp.take(offsets, picks)[:, None]).reshape(group * block)
        others = jnp.transpose(blocks[:, 1:, :], (1, 0, 2)).reshape(3, group * block)
        valid = (others[0] >= 0) & jnp.repeat(live, block)
        clamped = jnp.maximum(others, 0)
        terms = contributions(first_modes, clamped, clamped, valid, eig, freq, eig, freq, phi, cells)
        return rates.at[first_modes].add(terms)
    return lax.fori_loop(0, rounds, one_round, jnp.zeros((eig.shape[1],), jnp.float32))
```

```python
import functools
import math

import jax
import jax.numpy as jnp
from jax import lax
from jax.experimental import pallas as pl
from jax.experimental.pallas import tpu as pltpu
from jax.sharding import PartitionSpec as P

QMESH = 16
LANES = 128
PAIR = 2
smearing = 0.5


def outer_rows(first, second, branches):
    count = first.shape[1]
    twice = 2 * branches
    second_re = jnp.concatenate([second[:branches]] * 2, axis=0)
    second_im = jnp.concatenate([second[branches:]] * 2, axis=0)
    upper = lax.broadcasted_iota(jnp.int32, (twice, count), 0) < branches
    real, imag = [], []
    for a in range(0, branches, 2):
        first_re = jnp.where(upper, first[a : a + 1], first[a + 1 : a + 2])
        first_im = jnp.where(
            upper, first[branches + a : branches + a + 1], first[branches + a + 1 : branches + a + 2]
        )
        real.append(first_re * second_re - first_im * second_im)
        imag.append(first_re * second_im + first_im * second_re)
    return jnp.concatenate(real, axis=0), jnp.concatenate(imag, axis=0)


def look_up(table, modes, comps):
    width = table.shape[1]
    highs = table.shape[0] // (comps + 1)
    count = modes.shape[1]
    low = jnp.bitwise_and(modes, width - 1)
    high = lax.shift_right_logical(modes, width.bit_length() - 1)
    hot = jnp.where(
        lax.broadcasted_iota(jnp.int32, (width, count), 0) == low, 1.0, 0.0
    ).astype(jnp.bfloat16)
    found = jnp.dot(table[...], hot, preferred_element_type=jnp.float32)
    vectors = found[:comps]
    for h in range(1, highs):
        vectors = jnp.where(high == h, found[h * comps : (h + 1) * comps], vectors)
    rows = lax.broadcasted_iota(jnp.int32, (highs, count), 0)
    freqs = jnp.sum(
        jnp.where(rows == high, found[highs * comps :], 0.0), axis=0, keepdims=True
    )
    return vectors, freqs


def phases(others, cells, branches):
    points = [
        ((m.astype(jnp.float32) + 0.5) * (1.0 / branches)).astype(jnp.int32) for m in others
    ]
    bits = QMESH.bit_length() - 1
    shift = None
    for which, point in enumerate(points):
        coords = [
            lax.shift_right_logical(point, 2 * bits),
            jnp.bitwise_and(lax.shift_right_logical(point, bits), QMESH - 1),
            jnp.bitwise_and(point, QMESH - 1),
        ]
        for axis_c in range(3):
            at = 3 * which + axis_c
            move = cells[:, at : at + 1] * coords[axis_c]
            if shift is None:
                shift = move
            elif which == 0:
                shift = shift + move
            else:
                shift = shift - move
    turn = jnp.bitwise_and(shift, QMESH - 1)

    def cosine_of(steps):
        value = jnp.ones(steps.shape, jnp.float32)
        for t in range(1, QMESH):
            value = jnp.where(steps == t, math.cos(2.0 * math.pi * t / QMESH), value)
        return value

    return cosine_of(turn), cosine_of(jnp.bitwise_and(turn - QMESH // 4, QMESH - 1))


def rounds_kernel(
    workers, tallies, pool, table, own_table, phi, cells, out, order, total_rows
):
    held = pool.shape[0]
    block = pool.shape[2]
    per_source = held // workers
    pairs = phi.shape[0]
    branches = math.isqrt(pairs)
    comps = 2 * branches
    clusters = phi.shape[1] // pairs
    here = lax.axis_index("wa")

    def list_one(at, filled):
        source = at // per_source
        slot = (at % per_source) * workers + lax.rem(here - source + workers, workers)
        order[filled] = at
        return filled + (slot < tallies[0, source]).astype(jnp.int32)

    total = lax.fori_loop(0, held, list_one, jnp.int32(0))
    total_rows[...] = jnp.zeros_like(total_rows)
    span = out.shape[0] // workers
    padded = total_rows.shape[0] // workers
    count = PAIR * block

    def one_round(step, carry):
        picked, alive = [], []
        for p in range(PAIR):
            at = step * PAIR + p
            live = at < total
            picked.append(pool[order[jnp.minimum(at, total - 1)]])
            alive.append(jnp.full((1, block), live.astype(jnp.int32)))
        blocks = jnp.concatenate(picked, axis=1)
        live = jnp.concatenate(alive, axis=1)
        first_modes = blocks[0:1]
        valid = (blocks[1:2] >= 0) & (live > 0)
        others = [jnp.maximum(blocks[k : k + 1], 0) for k in (1, 2, 3)]
        first_vec, first_freq = look_up(own_table, first_modes, comps)
        vectors, freqs = look_up(table, jnp.concatenate(others, axis=1), comps)
        second_vec, third_vec, fourth_vec = (
            vectors[:, k * count : (k + 1) * count] for k in range(3)
        )
        f2, f3, f4 = (freqs[:, k * count : (k + 1) * count] for k in range(3))
        far_re, far_im = outer_rows(third_vec, fourth_vec, branches)
        cosine, sine = phases(others, cells[...], branches)
        wide_re, wide_im = [], []
        for k in range(clusters):
            c, s = cosine[k : k + 1], sine[k : k + 1]
            wide_re.append((c * far_re + s * far_im).astype(jnp.bfloat16))
            wide_im.append((s * far_re - c * far_im).astype(jnp.bfloat16))
        wide = jnp.concatenate(
            [jnp.concatenate(wide_re, axis=0), jnp.concatenate(wide_im, axis=0)], axis=1
        )
        weighted = jnp.dot(phi[...], wide, preferred_element_type=jnp.float32)
        weighted_re, weighted_im = weighted[:, :count], weighted[:, count:]
        near_re, near_im = outer_rows(first_vec, second_vec, branches)
        value_re = jnp.sum(near_re * weighted_re - near_im * weighted_im, axis=0, keepdims=True)
        value_im = jnp.sum(near_re * weighted_im + near_im * weighted_re, axis=0, keepdims=True)
        mismatch = (first_freq + f2 - f3 - f4) * (1.0 / smearing)
        g1, g2, g3, g4 = (jnp.exp(f) for f in (first_freq, f2, f3, f4))
        scale = 1.0 / (smearing * math.sqrt(math.pi))
        upper = g2 * (g1 - 1.0) * jnp.exp(-(mismatch * mismatch)) * scale
        lower = (g2 - 1.0) * (g3 - 1.0) * (g4 - 1.0) * (first_freq * f2 * f3 * f4)
        term = jnp.where(
            valid, (value_re * value_re + value_im * value_im) * upper / lower, 0.0
        )
        high = lax.shift_right_logical(first_modes, LANES.bit_length() - 1)
        holder = ((high.astype(jnp.float32) + 0.5) * (1.0 / span)).astype(jnp.int32)
        row = holder * padded + (high - holder * span)
        row_hot = jnp.where(
            lax.broadcasted_iota(jnp.int32, (workers * padded, count), 0) == row, 1.0, 0.0
        ).astype(jnp.bfloat16)
        lane = lax.broadcasted_iota(jnp.int32, (LANES, count), 0) == jnp.bitwise_and(
            first_modes, LANES - 1
        )
        big = term.astype(jnp.bfloat16).astype(jnp.float32)
        parts = jnp.concatenate(
            [jnp.where(lane, big, 0.0), jnp.where(lane, term - big, 0.0)], axis=0
        ).astype(jnp.bfloat16)
        both = lax.dot_general(
            row_hot, parts, (((1,), (1,)), ((), ())), preferred_element_type=jnp.float32
        )
        total_rows[...] += both[:, :LANES] + both[:, LANES:]
        return carry

    lax.fori_loop(0, (total + PAIR - 1) // PAIR, one_round, 0)
    for w in range(workers):
        out[w * span : (w + 1) * span] = total_rows[w * padded : w * padded + span]


def body(quartets, counts, eig, freq, phi, cells):
    comps, local_modes = eig.shape
    workers = lax.axis_size("wa")
    held, _, block = quartets.shape
    per_dest = held // workers
    width = math.gcd(local_modes, 1024)
    highs = local_modes // width
    own = jnp.transpose(eig.reshape(comps, highs, width), (1, 0, 2)).reshape(highs * comps, width)
    own_freq = freq.reshape(highs, width)
    own_table = jnp.concatenate([own, own_freq], axis=0)
    table = jnp.concatenate(
        [
            lax.all_gather(own, "pb", axis=0, tiled=True),
            lax.all_gather(own_freq, "pb", axis=0, tiled=True),
        ],
        axis=0,
    )
    dealt = jnp.roll(
        quartets.reshape(per_dest, workers, 4, block), lax.axis_index("wa"), axis=1
    )
    dealt = jnp.transpose(dealt, (1, 0, 2, 3))
    tallies = jnp.full((1, workers), counts[0], jnp.int32)
    pool = lax.all_to_all(dealt, "wa", split_axis=0, concat_axis=0, tiled=True)
    tallies = lax.all_to_all(tallies, "wa", split_axis=1, concat_axis=1, tiled=True)
    rows = local_modes // LANES
    padded = -(-(rows // workers) // 8) * 8
    vmem = pl.BlockSpec(memory_space=pltpu.VMEM)
    partial_value = pl.pallas_call(
        functools.partial(rounds_kernel, workers),
        out_shape=jax.ShapeDtypeStruct((rows, LANES), jnp.float32),
        in_specs=[pl.BlockSpec(memory_space=pltpu.SMEM)] + [vmem] * 5,
        out_specs=vmem,
        scratch_shapes=[
            pltpu.SMEM((held + 1,), jnp.int32),
            pltpu.VMEM((workers * padded, LANES), jnp.float32),
        ],
        compiler_params=pltpu.CompilerParams(vmem_limit_bytes=48 << 20),
        name="rounds",
    )(tallies, pool.reshape(held, 4, block), table, own_table, phi, cells)
    return lax.psum_scatter(
        partial_value.reshape(local_modes), "wa", scatter_dimension=0, tiled=True
    )


def solution(mesh):
    placed = (P(("pb", "wa"), None, None), P(("pb", "wa")), P(None, "pb"), P("pb"), P(), P())
    return jax.shard_map(
        body, mesh=mesh, in_specs=placed, out_specs=P(("pb", "wa")), check_vma=False
    )
```

```python
import functools
import math

import jax
import jax.numpy as jnp
from jax import lax
from jax.experimental import pallas as pl
from jax.experimental.pallas import tpu as pltpu
from jax.sharding import PartitionSpec as P

QMESH = 16
LANES = 128
MESH = pl.DeviceIdType.MESH
PAIR = 2
smearing = 0.5


def rows_of(comps, highs):
    return highs * comps + -(-highs // 8) * 8


def outer_rows(first, second, branches):
    count = first.shape[1]
    twice = 2 * branches
    second_re = jnp.concatenate([second[:branches]] * 2, axis=0)
    second_im = jnp.concatenate([second[branches:]] * 2, axis=0)
    upper = lax.broadcasted_iota(jnp.int32, (twice, count), 0) < branches
    real, imag = [], []
    for a in range(0, branches, 2):
        first_re = jnp.where(upper, first[a : a + 1], first[a + 1 : a + 2])
        first_im = jnp.where(
            upper, first[branches + a : branches + a + 1], first[branches + a + 1 : branches + a + 2]
        )
        real.append(first_re * second_re - first_im * second_im)
        imag.append(first_re * second_im + first_im * second_re)
    return jnp.concatenate(real, axis=0), jnp.concatenate(imag, axis=0)


def look_up(found, modes, comps, width, highs):
    count = modes.shape[1]
    owned = rows_of(comps, highs)
    high = lax.shift_right_logical(modes, width.bit_length() - 1)
    tail = owned - highs * comps
    rows = lax.broadcasted_iota(jnp.int32, (tail, count), 0)
    rows = jnp.where(rows < highs, rows, -found.shape[0])
    vectors, freqs = None, None
    for owner in range(found.shape[0] // owned):
        base = owner * owned
        for j in range(highs):
            part = found[base + j * comps : base + (j + 1) * comps]
            at = owner * highs + j
            vectors = part if vectors is None else jnp.where(high == at, part, vectors)
        part = found[base + highs * comps : base + owned]
        freqs = jnp.where(
            rows == high - owner * highs, part, 0.0 if freqs is None else freqs
        )
    return vectors, jnp.sum(freqs, axis=0, keepdims=True)


def one_hot(modes, width):
    low = jnp.bitwise_and(modes, width - 1)
    return jnp.where(
        lax.broadcasted_iota(jnp.int32, (width, modes.shape[1]), 0) == low, 1.0, 0.0
    ).astype(jnp.bfloat16)


def phases(others, cells, branches):
    points = [
        ((m.astype(jnp.float32) + 0.5) * (1.0 / branches)).astype(jnp.int32) for m in others
    ]
    bits = QMESH.bit_length() - 1
    shift = None
    for which, point in enumerate(points):
        coords = [
            lax.shift_right_logical(point, 2 * bits),
            jnp.bitwise_and(lax.shift_right_logical(point, bits), QMESH - 1),
            jnp.bitwise_and(point, QMESH - 1),
        ]
        for axis_c in range(3):
            at = 3 * which + axis_c
            move = cells[:, at : at + 1] * coords[axis_c]
            if shift is None:
                shift = move
            elif which == 0:
                shift = shift + move
            else:
                shift = shift - move
    turn = jnp.bitwise_and(shift, QMESH - 1)

    def cosine_of(steps):
        value = jnp.ones(steps.shape, jnp.float32)
        for t in range(1, QMESH):
            value = jnp.where(steps == t, math.cos(2.0 * math.pi * t / QMESH), value)
        return value

    return cosine_of(turn), cosine_of(jnp.bitwise_and(turn - QMESH // 4, QMESH - 1))


def rounds_kernel(
    workers, highs, tallies, pool, table, phi, cells, total_rows, order
):
    held = pool.shape[0]
    block = pool.shape[2]
    per_source = held // workers
    pairs = phi.shape[0]
    branches = math.isqrt(pairs)
    comps = 2 * branches
    clusters = phi.shape[1] // pairs
    here = lax.axis_index("wa")

    def list_one(at, filled):
        source = at // per_source
        slot = (at % per_source) * workers + lax.rem(here - source + workers, workers)
        order[filled] = at
        return filled + (slot < tallies[source, 0, 0]).astype(jnp.int32)

    total = lax.fori_loop(0, held, list_one, jnp.int32(0))
    total_rows[...] = jnp.zeros_like(total_rows)
    width = table.shape[1]
    owned = rows_of(comps, highs)
    own_rows = pl.ds(pl.multiple_of(lax.axis_index("pb") * owned, 8), owned)
    lanes = math.gcd(highs * width // workers, LANES)
    span = highs * width // workers // lanes
    padded = total_rows.shape[0] // workers
    count = PAIR * block

    def one_round(step, carry):
        picked, alive = [], []
        for p in range(PAIR):
            at = step * PAIR + p
            live = at < total
            picked.append(pool[order[jnp.minimum(at, total - 1)]])
            alive.append(jnp.full((1, block), live.astype(jnp.int32)))
        blocks = jnp.concatenate(picked, axis=1)
        live = jnp.concatenate(alive, axis=1)
        first_modes = blocks[0:1]
        valid = (blocks[1:2] >= 0) & (live > 0)
        others = [jnp.maximum(blocks[k : k + 1], 0) for k in (1, 2, 3)]
        found = jnp.dot(
            table[own_rows], one_hot(first_modes, width), preferred_element_type=jnp.float32
        )
        first_vec, first_freq = look_up(found, first_modes, comps, width, highs)
        joined = jnp.concatenate(others, axis=1)
        found = jnp.dot(
            table[...], one_hot(joined, width), preferred_element_type=jnp.float32
        )
        vectors, freqs = look_up(found, joined, comps, width, highs)
        second_vec, third_vec, fourth_vec = (
            vectors[:, k * count : (k + 1) * count] for k in range(3)
        )
        f2, f3, f4 = (freqs[:, k * count : (k + 1) * count] for k in range(3))
        far_re, far_im = outer_rows(third_vec, fourth_vec, branches)
        cosine, sine = phases(others, cells[...], branches)
        wide_re, wide_im = [], []
        for k in range(clusters):
            c, s = cosine[k : k + 1], sine[k : k + 1]
            wide_re.append((c * far_re + s * far_im).astype(jnp.bfloat16))
            wide_im.append((s * far_re - c * far_im).astype(jnp.bfloat16))
        wide = jnp.concatenate(
            [jnp.concatenate(wide_re, axis=0), jnp.concatenate(wide_im, axis=0)], axis=1
        )
        weighted = jnp.dot(phi[...], wide, preferred_element_type=jnp.float32)
        weighted_re, weighted_im = weighted[:, :count], weighted[:, count:]
        near_re, near_im = outer_rows(first_vec, second_vec, branches)
        value_re = jnp.sum(near_re * weighted_re - near_im * weighted_im, axis=0, keepdims=True)
        value_im = jnp.sum(near_re * weighted_im + near_im * weighted_re, axis=0, keepdims=True)
        mismatch = (first_freq + f2 - f3 - f4) * (1.0 / smearing)
        g1, g2, g3, g4 = (jnp.exp(f) for f in (first_freq, f2, f3, f4))
        scale = 1.0 / (smearing * math.sqrt(math.pi))
        upper = g2 * (g1 - 1.0) * jnp.exp(-(mismatch * mismatch)) * scale
        lower = (g2 - 1.0) * (g3 - 1.0) * (g4 - 1.0) * (first_freq * f2 * f3 * f4)
        term = jnp.where(
            valid, (value_re * value_re + value_im * value_im) * upper / lower, 0.0
        )
        high = lax.shift_right_logical(first_modes, lanes.bit_length() - 1)
        holder = ((high.astype(jnp.float32) + 0.5) * (1.0 / span)).astype(jnp.int32)
        row = holder * padded + (high - holder * span)
        row_hot = jnp.where(
            lax.broadcasted_iota(jnp.int32, (workers * padded, count), 0) == row, 1.0, 0.0
        ).astype(jnp.bfloat16)
        lane = lax.broadcasted_iota(jnp.int32, (LANES, count), 0) == jnp.bitwise_and(
            first_modes, lanes - 1
        )
        big = term.astype(jnp.bfloat16).astype(jnp.float32)
        parts = jnp.concatenate(
            [jnp.where(lane, big, 0.0), jnp.where(lane, term - big, 0.0)], axis=0
        ).astype(jnp.bfloat16)
        both = lax.dot_general(
            row_hot, parts, (((1,), (1,)), ((), ())), preferred_element_type=jnp.float32
        )
        total_rows[...] += both[:, :LANES] + both[:, LANES:]
        return carry

    lax.fori_loop(0, (total + PAIR - 1) // PAIR, one_round, 0)


def flipped(index, bits):
    value, bit = 0, 1
    while bit <= bits:
        digit = (index // bit) % 2
        value = value + bit * ((digit + 1) % 2 if bits & bit else digit)
        bit *= 2
    return value + (index // bit) * bit


def gather_kernel(
    owners, workers, highs, eig, freq, quartets, counts, table, pool, tallies,
    local_sem, give_send, give_recv, pass_send, pass_recv, deal_send, deal_recv,
    tally_send, tally_recv,
):
    group, here = lax.axis_index("pb"), lax.axis_index("wa")
    comps = eig.shape[0]
    width = table.shape[1]
    owned = rows_of(comps, highs)
    pieces = give_send.shape[1]
    half = width // 2
    piece = half // pieces
    core = here % 2
    sibling = {"wa": flipped(here, 1)}
    even = owners & (owners - 1) == 0

    def sent_to(k):
        return flipped(group, k) if even else (group + k) % owners

    def come_from(k):
        return flipped(group, k) if even else (group + owners - k) % owners

    def peer(k):
        return (here + k) % workers

    base = pl.multiple_of(group * owned, 8)
    local = [
        pltpu.make_async_copy(
            eig.at[:, pl.ds(j * width, width)],
            table.at[pl.ds(base + j * comps, comps)],
            local_sem.at[j],
        )
        for j in range(highs)
    ]
    local.append(
        pltpu.make_async_copy(
            freq,
            table.at[pl.ds(base + highs * comps, owned - highs * comps)],
            local_sem.at[highs],
        )
    )
    late = [
        pltpu.make_async_copy(quartets.at[:, 0], pool.at[here], local_sem.at[highs + 1]),
        pltpu.make_async_copy(counts, tallies.at[here], local_sem.at[highs + 2]),
    ]
    for copy in local + late:
        copy.start()

    barrier = pltpu.get_barrier_semaphore()
    for k in range(1, owners):
        pl.semaphore_signal(barrier, inc=1, device_id={"pb": sent_to(k)}, device_id_type=MESH)
    for k in range(1, workers):
        pl.semaphore_signal(barrier, inc=1, device_id={"wa": peer(k)}, device_id_type=MESH)
    pl.semaphore_wait(barrier, owners + workers - 2)

    for copy in local:
        copy.wait()

    def columns(side, q):
        return pl.ds(pl.multiple_of(side * half + q * piece, LANES), piece)

    def rows(owner):
        return pl.ds(pl.multiple_of(owner * owned, 8), owned)

    order = sorted(range(1, owners), key=lambda k: -bin(k).count("1"))
    waits = []
    gives = {}
    for q in range(pieces):
        for k in order:
            spot = table.at[rows(group), columns(core, q)]
            gives[q, k] = pltpu.make_async_remote_copy(
                src_ref=spot,
                dst_ref=spot,
                send_sem=give_send.at[k - 1, q],
                recv_sem=give_recv.at[k - 1, q],
                device_id={"pb": sent_to(k)},
                device_id_type=MESH,
            )
            gives[q, k].start()
    for k in range(1, workers):
        deal = pltpu.make_async_remote_copy(
            src_ref=quartets.at[:, k],
            dst_ref=pool.at[here],
            send_sem=deal_send.at[k - 1],
            recv_sem=deal_recv.at[k - 1],
            device_id={"wa": peer(k)},
            device_id_type=MESH,
        )
        tally = pltpu.make_async_remote_copy(
            src_ref=counts,
            dst_ref=tallies.at[here],
            send_sem=tally_send.at[k - 1],
            recv_sem=tally_recv.at[k - 1],
            device_id={"wa": peer(k)},
            device_id_type=MESH,
        )
        deal.start()
        tally.start()
        waits += [deal, tally]
    for q in range(pieces):
        for k in order:
            gives[q, k].wait_recv()
            spot = table.at[rows(come_from(k)), columns(core, q)]
            onward = pltpu.make_async_remote_copy(
                src_ref=spot,
                dst_ref=spot,
                send_sem=pass_send.at[k - 1, q],
                recv_sem=pass_recv.at[k - 1, q],
                device_id=sibling,
                device_id_type=MESH,
            )
            onward.start()
            waits.append(onward)
    for copy in late + waits:
        copy.wait()
    for copy in gives.values():
        copy.wait_send()


def reduce_kernel(workers, terms, out, landed, send_sem, recv_sem):
    here = lax.axis_index("wa")
    padded = landed.shape[1]
    barrier = pltpu.get_barrier_semaphore()
    for k in range(1, workers):
        pl.semaphore_signal(
            barrier, inc=1, device_id={"wa": (here + k) % workers}, device_id_type=MESH
        )
    pl.semaphore_wait(barrier, workers - 1)
    copies = []
    for k in range(1, workers):
        to = (here + k) % workers
        copy = pltpu.make_async_remote_copy(
            src_ref=terms.at[pl.ds(pl.multiple_of(to * padded, 8), padded)],
            dst_ref=landed.at[k - 1],
            send_sem=send_sem.at[k - 1],
            recv_sem=recv_sem.at[k - 1],
            device_id={"wa": to},
            device_id_type=MESH,
        )
        copy.start()
        copies.append(copy)
    value = terms[pl.ds(pl.multiple_of(here * padded, 8), padded)]
    for k, copy in enumerate(copies):
        copy.wait_recv()
        value = value + landed[k]
    out[...] = value[: out.shape[0]]
    for copy in copies:
        copy.wait_send()


def body(quartets, counts, eig, freq, phi, cells):
    comps, local_modes = eig.shape
    owners, workers = lax.axis_size("pb"), lax.axis_size("wa")
    held, _, block = quartets.shape
    per_dest = held // workers
    width = math.gcd(local_modes, 1024)
    highs = local_modes // width
    owned = rows_of(comps, highs)
    lanes = math.gcd(local_modes // workers, LANES)
    span = local_modes // workers // lanes
    padded = -(-span // 8) * 8
    vmem = pl.BlockSpec(memory_space=pltpu.VMEM)
    hbm = pl.BlockSpec(memory_space=pl.ANY)
    smem = pl.BlockSpec(memory_space=pltpu.SMEM)
    tail = owned - highs * comps
    freq_rows = jnp.pad(freq.reshape(highs, width), ((0, tail - highs), (0, 0)))
    own_deal = quartets.reshape(per_dest, workers, 4, block)
    pieces = 2
    dma = pltpu.SemaphoreType.DMA
    table, pool, tallies = pl.pallas_call(
        functools.partial(gather_kernel, owners, workers, highs),
        out_shape=[
            jax.ShapeDtypeStruct((owners * owned, width), eig.dtype),
            jax.ShapeDtypeStruct((workers, per_dest, 4, block), jnp.int32),
            jax.ShapeDtypeStruct((workers, 1, LANES), jnp.int32),
        ],
        in_specs=[hbm] * 3 + [vmem],
        out_specs=[vmem] * 3,
        scratch_shapes=[dma((highs + 3,))]
        + [dma((owners - 1, pieces))] * 4
        + [dma((workers - 1,))] * 4,
        compiler_params=pltpu.CompilerParams(
            collective_id=0, has_side_effects=True, vmem_limit_bytes=48 << 20
        ),
        name="gather",
    )(eig, freq_rows, own_deal, jnp.full((1, LANES), counts[0], jnp.int32))
    terms = pl.pallas_call(
        functools.partial(rounds_kernel, workers, highs),
        out_shape=jax.ShapeDtypeStruct((workers * padded, LANES), jnp.float32),
        in_specs=[smem] + [vmem] * 4,
        out_specs=vmem,
        scratch_shapes=[pltpu.SMEM((held + 1,), jnp.int32)],
        compiler_params=pltpu.CompilerParams(vmem_limit_bytes=48 << 20),
        name="rounds",
    )(tallies, pool.reshape(held, 4, block), table, phi, cells)
    rates = pl.pallas_call(
        functools.partial(reduce_kernel, workers),
        out_shape=jax.ShapeDtypeStruct((span, LANES), jnp.float32),
        in_specs=[vmem],
        out_specs=vmem,
        scratch_shapes=[
            pltpu.VMEM((workers - 1, padded, LANES), jnp.float32),
            dma((workers - 1,)),
            dma((workers - 1,)),
        ],
        compiler_params=pltpu.CompilerParams(collective_id=1, has_side_effects=True),
        name="reduce",
    )(terms)
    return rates[:, :lanes].reshape(span * lanes)


def solution(mesh):
    placed = (P(("pb", "wa"), None, None), P(("pb", "wa")), P(None, "pb"), P("pb"), P(), P())
    return jax.shard_map(
        body, mesh=mesh, in_specs=placed, out_specs=P(("pb", "wa")), check_vma=False
    )
```

```python
import functools
import math

import jax
import jax.numpy as jnp
from jax import lax
from jax.experimental import pallas as pl
from jax.experimental.pallas import tpu as pltpu
from jax.sharding import PartitionSpec as P

QMESH = 16
LANES = 128
MESH = pl.DeviceIdType.MESH
PAIR = 2
smearing = 0.5


def rows_of(comps, highs):
    return highs * comps + -(-highs // 8) * 8


def outer_rows(first, second, branches):
    count = first.shape[1]
    twice = 2 * branches
    second_re = jnp.concatenate([second[:branches]] * 2, axis=0)
    second_im = jnp.concatenate([second[branches:]] * 2, axis=0)
    upper = lax.broadcasted_iota(jnp.int32, (twice, count), 0) < branches
    real, imag = [], []
    for a in range(0, branches, 2):
        first_re = jnp.where(upper, first[a : a + 1], first[a + 1 : a + 2])
        first_im = jnp.where(
            upper, first[branches + a : branches + a + 1], first[branches + a + 1 : branches + a + 2]
        )
        real.append(first_re * second_re - first_im * second_im)
        imag.append(first_re * second_im + first_im * second_re)
    return jnp.concatenate(real, axis=0), jnp.concatenate(imag, axis=0)


def look_up(found, modes, comps, width, highs):
    count = modes.shape[1]
    owned = rows_of(comps, highs)
    high = lax.shift_right_logical(modes, width.bit_length() - 1)
    tail = owned - highs * comps
    rows = lax.broadcasted_iota(jnp.int32, (tail, count), 0)
    rows = jnp.where(rows < highs, rows, -found.shape[0])
    vectors, freqs = None, None
    for owner in range(found.shape[0] // owned):
        base = owner * owned
        for j in range(highs):
            part = found[base + j * comps : base + (j + 1) * comps]
            at = owner * highs + j
            vectors = part if vectors is None else jnp.where(high == at, part, vectors)
        part = found[base + highs * comps : base + owned]
        freqs = jnp.where(
            rows == high - owner * highs, part, 0.0 if freqs is None else freqs
        )
    return vectors, jnp.sum(freqs, axis=0, keepdims=True)


def one_hot(modes, width):
    low = jnp.bitwise_and(modes, width - 1)
    return jnp.where(
        lax.broadcasted_iota(jnp.int32, (width, modes.shape[1]), 0) == low, 1.0, 0.0
    ).astype(jnp.bfloat16)


def phases(others, cells, branches):
    points = [
        ((m.astype(jnp.float32) + 0.5) * (1.0 / branches)).astype(jnp.int32) for m in others
    ]
    bits = QMESH.bit_length() - 1
    shift = None
    for which, point in enumerate(points):
        coords = [
            lax.shift_right_logical(point, 2 * bits),
            jnp.bitwise_and(lax.shift_right_logical(point, bits), QMESH - 1),
            jnp.bitwise_and(point, QMESH - 1),
        ]
        for axis_c in range(3):
            at = 3 * which + axis_c
            move = cells[:, at : at + 1] * coords[axis_c]
            if shift is None:
                shift = move
            elif which == 0:
                shift = shift + move
            else:
                shift = shift - move
    turn = jnp.bitwise_and(shift, QMESH - 1)

    def cosine_of(steps):
        value = jnp.ones(steps.shape, jnp.float32)
        for t in range(1, QMESH):
            value = jnp.where(steps == t, math.cos(2.0 * math.pi * t / QMESH), value)
        return value

    return cosine_of(turn), cosine_of(jnp.bitwise_and(turn - QMESH // 4, QMESH - 1))


def rounds_kernel(
    workers, highs, tallies, pool, table, phi, cells, total_rows, order
):
    held = pool.shape[0]
    block = pool.shape[2]
    per_source = held // workers
    pairs = phi.shape[0]
    branches = math.isqrt(pairs)
    comps = 2 * branches
    clusters = phi.shape[1] // pairs
    here = lax.axis_index("wa")

    def list_one(at, filled):
        source = at // per_source
        slot = (at % per_source) * workers + lax.rem(here - source + workers, workers)
        order[filled] = at
        return filled + (slot < tallies[source, 0, 0]).astype(jnp.int32)

    total = lax.fori_loop(0, held, list_one, jnp.int32(0))
    total_rows[...] = jnp.zeros_like(total_rows)
    width = table.shape[1]
    owned = rows_of(comps, highs)
    own_rows = pl.ds(pl.multiple_of(lax.axis_index("pb") * owned, 8), owned)
    lanes = math.gcd(highs * width // workers, LANES)
    span = highs * width // workers // lanes
    padded = total_rows.shape[0] // workers
    count = PAIR * block

    def looked_up(step):
        picked, alive = [], []
        for p in range(PAIR):
            at = step * PAIR + p
            live = at < total
            picked.append(pool[order[jnp.maximum(jnp.minimum(at, total - 1), 0)]])
            alive.append(jnp.full((1, block), live.astype(jnp.int32)))
        blocks = jnp.concatenate(picked, axis=1)
        live = jnp.concatenate(alive, axis=1)
        first_modes = blocks[0:1]
        valid = (blocks[1:2] >= 0) & (live > 0)
        others = [jnp.maximum(blocks[k : k + 1], 0) for k in (1, 2, 3)]
        found = jnp.dot(
            table[own_rows], one_hot(first_modes, width), preferred_element_type=jnp.float32
        )
        first_vec, first_freq = look_up(found, first_modes, comps, width, highs)
        joined = jnp.concatenate(others, axis=1)
        found = jnp.dot(
            table[...], one_hot(joined, width), preferred_element_type=jnp.float32
        )
        vectors, freqs = look_up(found, joined, comps, width, highs)
        cosine, sine = phases(others, cells[...], branches)
        return first_modes, valid.astype(jnp.int32), first_vec, first_freq, vectors, freqs, cosine, sine

    def add_up(looked):
        first_modes, valid, first_vec, first_freq, vectors, freqs, cosine, sine = looked
        second_vec, third_vec, fourth_vec = (
            vectors[:, k * count : (k + 1) * count] for k in range(3)
        )
        f2, f3, f4 = (freqs[:, k * count : (k + 1) * count] for k in range(3))
        far_re, far_im = outer_rows(third_vec, fourth_vec, branches)
        wide_re, wide_im = [], []
        for k in range(clusters):
            c, s = cosine[k : k + 1], sine[k : k + 1]
            wide_re.append((c * far_re + s * far_im).astype(jnp.bfloat16))
            wide_im.append((s * far_re - c * far_im).astype(jnp.bfloat16))
        wide = jnp.concatenate(
            [jnp.concatenate(wide_re, axis=0), jnp.concatenate(wide_im, axis=0)], axis=1
        )
        weighted = jnp.dot(phi[...], wide, preferred_element_type=jnp.float32)
        weighted_re, weighted_im = weighted[:, :count], weighted[:, count:]
        near_re, near_im = outer_rows(first_vec, second_vec, branches)
        value_re = jnp.sum(near_re * weighted_re - near_im * weighted_im, axis=0, keepdims=True)
        value_im = jnp.sum(near_re * weighted_im + near_im * weighted_re, axis=0, keepdims=True)
        mismatch = (first_freq + f2 - f3 - f4) * (1.0 / smearing)
        g1, g2, g3, g4 = (jnp.exp(f) for f in (first_freq, f2, f3, f4))
        scale = 1.0 / (smearing * math.sqrt(math.pi))
        upper = g2 * (g1 - 1.0) * jnp.exp(-(mismatch * mismatch)) * scale
        lower = (g2 - 1.0) * (g3 - 1.0) * (g4 - 1.0) * (first_freq * f2 * f3 * f4)
        term = jnp.where(
            valid > 0, (value_re * value_re + value_im * value_im) * upper / lower, 0.0
        )
        high = lax.shift_right_logical(first_modes, lanes.bit_length() - 1)
        holder = ((high.astype(jnp.float32) + 0.5) * (1.0 / span)).astype(jnp.int32)
        row = holder * padded + (high - holder * span)
        row_hot = jnp.where(
            lax.broadcasted_iota(jnp.int32, (workers * padded, count), 0) == row, 1.0, 0.0
        ).astype(jnp.bfloat16)
        lane = lax.broadcasted_iota(jnp.int32, (LANES, count), 0) == jnp.bitwise_and(
            first_modes, lanes - 1
        )
        big = term.astype(jnp.bfloat16).astype(jnp.float32)
        parts = jnp.concatenate(
            [jnp.where(lane, big, 0.0), jnp.where(lane, term - big, 0.0)], axis=0
        ).astype(jnp.bfloat16)
        both = lax.dot_general(
            row_hot, parts, (((1,), (1,)), ((), ())), preferred_element_type=jnp.float32
        )
        total_rows[...] += both[:, :LANES] + both[:, LANES:]

    def one_round(step, looked):
        following = looked_up(step)
        add_up(looked)
        return following

    rounds = (total + PAIR - 1) // PAIR
    add_up(lax.fori_loop(1, rounds, one_round, looked_up(0)))


def flipped(index, bits):
    value, bit = 0, 1
    while bit <= bits:
        digit = (index // bit) % 2
        value = value + bit * ((digit + 1) % 2 if bits & bit else digit)
        bit *= 2
    return value + (index // bit) * bit


def gather_kernel(
    owners, workers, highs, eig, freq, quartets, counts, table, pool, tallies,
    local_sem, give_send, give_recv, pass_send, pass_recv, deal_send, deal_recv,
    tally_send, tally_recv,
):
    group, here = lax.axis_index("pb"), lax.axis_index("wa")
    comps = eig.shape[0]
    width = table.shape[1]
    owned = rows_of(comps, highs)
    pieces = give_send.shape[1]
    even = owners & (owners - 1) == 0

    def sharers(k):
        far = even and bin(k).count("1") > 1 and workers % 4 == 0
        return 4 if far else 2

    def sent_to(k):
        return flipped(group, k) if even else (group + k) % owners

    def come_from(k):
        return flipped(group, k) if even else (group + owners - k) % owners

    def peer(k):
        return (here + k) % workers

    base = pl.multiple_of(group * owned, 8)
    local = [
        pltpu.make_async_copy(
            eig.at[:, pl.ds(j * width, width)],
            table.at[pl.ds(base + j * comps, comps)],
            local_sem.at[j],
        )
        for j in range(highs)
    ]
    local.append(
        pltpu.make_async_copy(
            freq,
            table.at[pl.ds(base + highs * comps, owned - highs * comps)],
            local_sem.at[highs],
        )
    )
    late = [
        pltpu.make_async_copy(quartets.at[:, 0], pool.at[here], local_sem.at[highs + 1]),
        pltpu.make_async_copy(counts, tallies.at[here], local_sem.at[highs + 2]),
    ]
    for copy in local + late:
        copy.start()

    barrier = pltpu.get_barrier_semaphore()
    for k in range(1, owners):
        pl.semaphore_signal(barrier, inc=1, device_id={"pb": sent_to(k)}, device_id_type=MESH)
    for k in range(1, workers):
        pl.semaphore_signal(barrier, inc=1, device_id={"wa": peer(k)}, device_id_type=MESH)
    pl.semaphore_wait(barrier, owners + workers - 2)

    for copy in local:
        copy.wait()

    def columns(k, q):
        part = width // sharers(k)
        piece = part // pieces
        return pl.ds(pl.multiple_of(here % sharers(k) * part + q * piece, LANES), piece)

    def rows(owner):
        return pl.ds(pl.multiple_of(owner * owned, 8), owned)

    order = sorted(range(1, owners), key=lambda k: -bin(k).count("1"))
    waits = []
    gives = {}
    turns = sorted(
        [(k, q) for q in range(pieces) for k in order], key=lambda turn: 4 - sharers(turn[0])
    )
    for k, q in turns:
            spot = table.at[rows(group), columns(k, q)]
            gives[q, k] = pltpu.make_async_remote_copy(
                src_ref=spot,
                dst_ref=spot,
                send_sem=give_send.at[k - 1, q],
                recv_sem=give_recv.at[k - 1, q],
                device_id={"pb": sent_to(k)},
                device_id_type=MESH,
            )
            gives[q, k].start()
    for k in range(1, workers):
        deal = pltpu.make_async_remote_copy(
            src_ref=quartets.at[:, k],
            dst_ref=pool.at[here],
            send_sem=deal_send.at[k - 1],
            recv_sem=deal_recv.at[k - 1],
            device_id={"wa": peer(k)},
            device_id_type=MESH,
        )
        tally = pltpu.make_async_remote_copy(
            src_ref=counts,
            dst_ref=tallies.at[here],
            send_sem=tally_send.at[k - 1],
            recv_sem=tally_recv.at[k - 1],
            device_id={"wa": peer(k)},
            device_id_type=MESH,
        )
        deal.start()
        tally.start()
        waits += [deal, tally]
    for k, q in turns:
            gives[q, k].wait_recv()
            spot = table.at[rows(come_from(k)), columns(k, q)]
            for j in range(1, sharers(k)):
                onward = pltpu.make_async_remote_copy(
                    src_ref=spot,
                    dst_ref=spot,
                    send_sem=pass_send.at[k - 1, q, j - 1],
                    recv_sem=pass_recv.at[k - 1, q, j - 1],
                    device_id={"wa": flipped(here, j)},
                    device_id_type=MESH,
                )
                onward.start()
                waits.append(onward)
    for copy in late + waits:
        copy.wait()
    for copy in gives.values():
        copy.wait_send()


def reduce_kernel(workers, terms, out, landed, send_sem, recv_sem):
    here = lax.axis_index("wa")
    padded = landed.shape[1]
    barrier = pltpu.get_barrier_semaphore()
    for k in range(1, workers):
        pl.semaphore_signal(
            barrier, inc=1, device_id={"wa": (here + k) % workers}, device_id_type=MESH
        )
    pl.semaphore_wait(barrier, workers - 1)
    copies = []
    for k in range(1, workers):
        to = (here + k) % workers
        copy = pltpu.make_async_remote_copy(
            src_ref=terms.at[pl.ds(pl.multiple_of(to * padded, 8), padded)],
            dst_ref=landed.at[k - 1],
            send_sem=send_sem.at[k - 1],
            recv_sem=recv_sem.at[k - 1],
            device_id={"wa": to},
            device_id_type=MESH,
        )
        copy.start()
        copies.append(copy)
    value = terms[pl.ds(pl.multiple_of(here * padded, 8), padded)]
    for k, copy in enumerate(copies):
        copy.wait_recv()
        value = value + landed[k]
    if len(out.shape) == 1:
        for r in range(out.shape[0] // LANES):
            out[r * LANES : (r + 1) * LANES] = value[r]
    else:
        out[...] = value[: out.shape[0]]
    for copy in copies:
        copy.wait_send()


def body(quartets, counts, eig, freq, phi, cells):
    comps, local_modes = eig.shape
    owners, workers = lax.axis_size("pb"), lax.axis_size("wa")
    held, _, block = quartets.shape
    per_dest = held // workers
    width = math.gcd(local_modes, 1024)
    highs = local_modes // width
    owned = rows_of(comps, highs)
    lanes = math.gcd(local_modes // workers, LANES)
    span = local_modes // workers // lanes
    padded = -(-span // 8) * 8
    vmem = pl.BlockSpec(memory_space=pltpu.VMEM)
    hbm = pl.BlockSpec(memory_space=pltpu.HBM)
    smem = pl.BlockSpec(memory_space=pltpu.SMEM)
    tail = owned - highs * comps
    freq_rows = jnp.pad(freq.reshape(highs, width), ((0, tail - highs), (0, 0)))
    own_deal = quartets.reshape(per_dest, workers, 4, block)
    pieces = 2
    dma = pltpu.SemaphoreType.DMA
    table, pool, tallies = pl.pallas_call(
        functools.partial(gather_kernel, owners, workers, highs),
        out_shape=[
            jax.ShapeDtypeStruct((owners * owned, width), eig.dtype),
            jax.ShapeDtypeStruct((workers, per_dest, 4, block), jnp.int32),
            jax.ShapeDtypeStruct((workers, 1, LANES), jnp.int32),
        ],
        in_specs=[hbm] * 3 + [vmem],
        out_specs=[vmem] * 3,
        scratch_shapes=[dma((highs + 3,))]
        + [dma((owners - 1, pieces))] * 2
        + [dma((owners - 1, pieces, 3))] * 2
        + [dma((workers - 1,))] * 4,
        compiler_params=pltpu.CompilerParams(
            collective_id=0, has_side_effects=True, vmem_limit_bytes=48 << 20
        ),
        name="gather",
    )(eig, freq_rows, own_deal, jnp.full((1, LANES), counts[0], jnp.int32))
    terms = pl.pallas_call(
        functools.partial(rounds_kernel, workers, highs),
        out_shape=jax.ShapeDtypeStruct((workers * padded, LANES), jnp.float32),
        in_specs=[smem] + [vmem] * 4,
        out_specs=vmem,
        scratch_shapes=[pltpu.SMEM((held + 1,), jnp.int32)],
        compiler_params=pltpu.CompilerParams(vmem_limit_bytes=48 << 20),
        name="rounds",
    )(tallies, pool.reshape(held, 4, block), table, phi, cells)
    rates = pl.pallas_call(
        functools.partial(reduce_kernel, workers),
        out_shape=jax.ShapeDtypeStruct(
            (span * LANES,) if lanes == LANES else (span, LANES), jnp.float32
        ),
        in_specs=[vmem],
        out_specs=vmem,
        scratch_shapes=[
            pltpu.VMEM((workers - 1, padded, LANES), jnp.float32),
            dma((workers - 1,)),
            dma((workers - 1,)),
        ],
        compiler_params=pltpu.CompilerParams(collective_id=1, has_side_effects=True),
        name="reduce",
    )(terms)
    return rates if lanes == LANES else rates[:, :lanes].reshape(span * lanes)


def solution(mesh):
    placed = (P(("pb", "wa"), None, None), P(("pb", "wa")), P(None, "pb"), P("pb"), P(), P())
    return jax.shard_map(
        body, mesh=mesh, in_specs=placed, out_specs=P(("pb", "wa")), check_vma=False
    )
```

```python
import functools
import math

import jax
import jax.numpy as jnp
from jax import lax
from jax.experimental import pallas as pl
from jax.experimental.pallas import tpu as pltpu
from jax.sharding import PartitionSpec as P

QMESH = 16
LANES = 128
MESH = pl.DeviceIdType.MESH
PAIR = 2
smearing = 0.5


def rows_of(comps, highs):
    return highs * comps + -(-highs // 8) * 8


def outer_rows(first, second, branches):
    count = first.shape[1]
    twice = 2 * branches
    second_re = jnp.concatenate([second[:branches]] * 2, axis=0)
    second_im = jnp.concatenate([second[branches:]] * 2, axis=0)
    upper = lax.broadcasted_iota(jnp.int32, (twice, count), 0) < branches
    real, imag = [], []
    for a in range(0, branches, 2):
        first_re = jnp.where(upper, first[a : a + 1], first[a + 1 : a + 2])
        first_im = jnp.where(
            upper, first[branches + a : branches + a + 1], first[branches + a + 1 : branches + a + 2]
        )
        real.append(first_re * second_re - first_im * second_im)
        imag.append(first_re * second_im + first_im * second_re)
    return jnp.concatenate(real, axis=0), jnp.concatenate(imag, axis=0)


def look_up(found, modes, comps, width, highs):
    count = modes.shape[1]
    owned = rows_of(comps, highs)
    high = lax.shift_right_logical(modes, width.bit_length() - 1)
    tail = owned - highs * comps
    rows = lax.broadcasted_iota(jnp.int32, (tail, count), 0)
    rows = jnp.where(rows < highs, rows, -found.shape[0])
    vectors, freqs = None, None
    for owner in range(found.shape[0] // owned):
        base = owner * owned
        for j in range(highs):
            part = found[base + j * comps : base + (j + 1) * comps]
            at = owner * highs + j
            vectors = part if vectors is None else jnp.where(high == at, part, vectors)
        part = found[base + highs * comps : base + owned]
        freqs = jnp.where(
            rows == high - owner * highs, part, 0.0 if freqs is None else freqs
        )
    return vectors, jnp.sum(freqs, axis=0, keepdims=True)


def one_hot(modes, width):
    low = jnp.bitwise_and(modes, width - 1)
    return jnp.where(
        lax.broadcasted_iota(jnp.int32, (width, modes.shape[1]), 0) == low, 1.0, 0.0
    ).astype(jnp.bfloat16)


def phases(others, cells, branches):
    points = [
        ((m.astype(jnp.float32) + 0.5) * (1.0 / branches)).astype(jnp.int32) for m in others
    ]
    bits = QMESH.bit_length() - 1
    shift = None
    for which, point in enumerate(points):
        coords = [
            lax.shift_right_logical(point, 2 * bits),
            jnp.bitwise_and(lax.shift_right_logical(point, bits), QMESH - 1),
            jnp.bitwise_and(point, QMESH - 1),
        ]
        for axis_c in range(3):
            at = 3 * which + axis_c
            move = cells[:, at : at + 1] * coords[axis_c]
            if shift is None:
                shift = move
            elif which == 0:
                shift = shift + move
            else:
                shift = shift - move
    turn = jnp.bitwise_and(shift, QMESH - 1)

    def cosine_of(steps):
        value = jnp.ones(steps.shape, jnp.float32)
        for t in range(1, QMESH):
            value = jnp.where(steps == t, math.cos(2.0 * math.pi * t / QMESH), value)
        return value

    return cosine_of(turn), cosine_of(jnp.bitwise_and(turn - QMESH // 4, QMESH - 1))


def rounds_kernel(
    workers, highs, tallies, pool, table, phi, cells, total_rows, order
):
    held = pool.shape[0]
    block = pool.shape[2]
    per_source = held // workers
    pairs = phi.shape[0]
    branches = math.isqrt(pairs)
    comps = 2 * branches
    clusters = phi.shape[1] // pairs
    here = lax.axis_index("wa")

    def list_one(at, filled):
        source = at // per_source
        slot = (at % per_source) * workers + lax.rem(here - source + workers, workers)
        order[filled] = at
        return filled + (slot < tallies[source, 0, 0]).astype(jnp.int32)

    total = lax.fori_loop(0, held, list_one, jnp.int32(0))
    total_rows[...] = jnp.zeros_like(total_rows)
    width = table.shape[1]
    owned = rows_of(comps, highs)
    own_rows = pl.ds(pl.multiple_of(lax.axis_index("pb") * owned, 8), owned)
    lanes = math.gcd(highs * width // workers, LANES)
    span = highs * width // workers // lanes
    padded = total_rows.shape[0] // workers
    count = PAIR * block

    def looked_up(step):
        picked, alive = [], []
        for p in range(PAIR):
            at = step * PAIR + p
            live = at < total
            picked.append(pool[order[jnp.maximum(jnp.minimum(at, total - 1), 0)]])
            alive.append(jnp.full((1, block), live.astype(jnp.int32)))
        blocks = jnp.concatenate(picked, axis=1)
        live = jnp.concatenate(alive, axis=1)
        first_modes = blocks[0:1]
        valid = (blocks[1:2] >= 0) & (live > 0)
        others = [jnp.maximum(blocks[k : k + 1], 0) for k in (1, 2, 3)]
        found = jnp.dot(
            table[own_rows], one_hot(first_modes, width), preferred_element_type=jnp.float32
        )
        first_vec, first_freq = look_up(found, first_modes, comps, width, highs)
        joined = jnp.concatenate(others, axis=1)
        found = jnp.dot(
            table[...], one_hot(joined, width), preferred_element_type=jnp.float32
        )
        vectors, freqs = look_up(found, joined, comps, width, highs)
        cosine, sine = phases(others, cells[...], branches)
        return first_modes, valid.astype(jnp.int32), first_vec, first_freq, vectors, freqs, cosine, sine

    def add_up(looked):
        first_modes, valid, first_vec, first_freq, vectors, freqs, cosine, sine = looked
        second_vec, third_vec, fourth_vec = (
            vectors[:, k * count : (k + 1) * count] for k in range(3)
        )
        f2, f3, f4 = (freqs[:, k * count : (k + 1) * count] for k in range(3))
        far_re, far_im = outer_rows(third_vec, fourth_vec, branches)
        wide_re, wide_im = [], []
        for k in range(clusters):
            c, s = cosine[k : k + 1], sine[k : k + 1]
            wide_re.append((c * far_re + s * far_im).astype(jnp.bfloat16))
            wide_im.append((s * far_re - c * far_im).astype(jnp.bfloat16))
        wide = jnp.concatenate(
            [jnp.concatenate(wide_re, axis=0), jnp.concatenate(wide_im, axis=0)], axis=1
        )
        weighted = jnp.dot(phi[...], wide, preferred_element_type=jnp.float32)
        weighted_re, weighted_im = weighted[:, :count], weighted[:, count:]
        near_re, near_im = outer_rows(first_vec, second_vec, branches)
        value_re = jnp.sum(near_re * weighted_re - near_im * weighted_im, axis=0, keepdims=True)
        value_im = jnp.sum(near_re * weighted_im + near_im * weighted_re, axis=0, keepdims=True)
        mismatch = (first_freq + f2 - f3 - f4) * (1.0 / smearing)
        g1, g2, g3, g4 = (jnp.exp(f) for f in (first_freq, f2, f3, f4))
        scale = 1.0 / (smearing * math.sqrt(math.pi))
        upper = g2 * (g1 - 1.0) * jnp.exp(-(mismatch * mismatch)) * scale
        lower = (g2 - 1.0) * (g3 - 1.0) * (g4 - 1.0) * (first_freq * f2 * f3 * f4)
        term = jnp.where(
            valid > 0, (value_re * value_re + value_im * value_im) * upper / lower, 0.0
        )
        high = lax.shift_right_logical(first_modes, lanes.bit_length() - 1)
        holder = ((high.astype(jnp.float32) + 0.5) * (1.0 / span)).astype(jnp.int32)
        row = holder * padded + (high - holder * span)
        row_hot = jnp.where(
            lax.broadcasted_iota(jnp.int32, (workers * padded, count), 0) == row, 1.0, 0.0
        ).astype(jnp.bfloat16)
        lane = lax.broadcasted_iota(jnp.int32, (LANES, count), 0) == jnp.bitwise_and(
            first_modes, lanes - 1
        )
        big = term.astype(jnp.bfloat16).astype(jnp.float32)
        parts = jnp.concatenate(
            [jnp.where(lane, big, 0.0), jnp.where(lane, term - big, 0.0)], axis=0
        ).astype(jnp.bfloat16)
        both = lax.dot_general(
            row_hot, parts, (((1,), (1,)), ((), ())), preferred_element_type=jnp.float32
        )
        total_rows[...] += both[:, :LANES] + both[:, LANES:]

    def one_round(step, looked):
        following = looked_up(step)
        add_up(looked)
        return following

    rounds = (total + PAIR - 1) // PAIR
    add_up(lax.fori_loop(1, rounds, one_round, looked_up(0)))


def flipped(index, bits):
    value, bit = 0, 1
    while bit <= bits:
        digit = (index // bit) % 2
        value = value + bit * ((digit + 1) % 2 if bits & bit else digit)
        bit *= 2
    return value + (index // bit) * bit


def gather_kernel(
    owners, workers, highs, eig, freq, quartets, counts, table, pool, tallies,
    local_sem, give_send, give_recv, pass_send, pass_recv, deal_send, deal_recv,
    tally_send, tally_recv,
):
    group, here = lax.axis_index("pb"), lax.axis_index("wa")
    comps = eig.shape[0]
    width = table.shape[1]
    owned = rows_of(comps, highs)
    pieces = give_send.shape[1]
    even = owners & (owners - 1) == 0

    def sharers(k):
        far = even and bin(k).count("1") > 1 and workers % 4 == 0
        return 4 if far else 2

    def sent_to(k):
        return flipped(group, k) if even else (group + k) % owners

    def come_from(k):
        return flipped(group, k) if even else (group + owners - k) % owners

    def peer(k):
        return (here + k) % workers

    base = pl.multiple_of(group * owned, 8)
    local = [
        pltpu.make_async_copy(
            eig.at[:, pl.ds(j * width, width)],
            table.at[pl.ds(base + j * comps, comps)],
            local_sem.at[j],
        )
        for j in range(highs)
    ]
    local.append(
        pltpu.make_async_copy(
            freq,
            table.at[pl.ds(base + highs * comps, owned - highs * comps)],
            local_sem.at[highs],
        )
    )
    late = [
        pltpu.make_async_copy(quartets.at[:, 0], pool.at[here], local_sem.at[highs + 1]),
        pltpu.make_async_copy(counts, tallies.at[here], local_sem.at[highs + 2]),
    ]
    for copy in local + late:
        copy.start()

    barrier = pltpu.get_barrier_semaphore()
    for k in range(1, owners):
        pl.semaphore_signal(barrier, inc=1, device_id={"pb": sent_to(k)}, device_id_type=MESH)
    for k in range(1, workers):
        pl.semaphore_signal(barrier, inc=1, device_id={"wa": peer(k)}, device_id_type=MESH)
    pl.semaphore_wait(barrier, owners + workers - 2)

    for copy in local:
        copy.wait()

    def columns(k, q):
        part = width // sharers(k)
        piece = part // pieces
        return pl.ds(pl.multiple_of(here % sharers(k) * part + q * piece, LANES), piece)

    def rows(owner):
        return pl.ds(pl.multiple_of(owner * owned, 8), owned)

    order = sorted(range(1, owners), key=lambda k: -bin(k).count("1"))
    waits = []
    gives = {}
    turns = sorted(
        [(k, q) for q in range(pieces) for k in order], key=lambda turn: 4 - sharers(turn[0])
    )
    for k, q in turns:
            spot = table.at[rows(group), columns(k, q)]
            gives[q, k] = pltpu.make_async_remote_copy(
                src_ref=spot,
                dst_ref=spot,
                send_sem=give_send.at[k - 1, q],
                recv_sem=give_recv.at[k - 1, q],
                device_id={"pb": sent_to(k)},
                device_id_type=MESH,
            )
            gives[q, k].start()
    for k in range(1, workers):
        deal = pltpu.make_async_remote_copy(
            src_ref=quartets.at[:, k],
            dst_ref=pool.at[here],
            send_sem=deal_send.at[k - 1],
            recv_sem=deal_recv.at[k - 1],
            device_id={"wa": peer(k)},
            device_id_type=MESH,
        )
        tally = pltpu.make_async_remote_copy(
            src_ref=counts,
            dst_ref=tallies.at[here],
            send_sem=tally_send.at[k - 1],
            recv_sem=tally_recv.at[k - 1],
            device_id={"wa": peer(k)},
            device_id_type=MESH,
        )
        deal.start()
        tally.start()
        waits += [deal, tally]
    for k, q in turns:
            gives[q, k].wait_recv()
            spot = table.at[rows(come_from(k)), columns(k, q)]
            for j in range(1, sharers(k)):
                onward = pltpu.make_async_remote_copy(
                    src_ref=spot,
                    dst_ref=spot,
                    send_sem=pass_send.at[k - 1, q, j - 1],
                    recv_sem=pass_recv.at[k - 1, q, j - 1],
                    device_id={"wa": flipped(here, j)},
                    device_id_type=MESH,
                )
                onward.start()
                waits.append(onward)
    for copy in late + waits:
        copy.wait()
    for copy in gives.values():
        copy.wait_send()


def reduce_kernel(workers, terms, out, landed, send_sem, recv_sem):
    here = lax.axis_index("wa")
    padded = landed.shape[1]
    barrier = pltpu.get_barrier_semaphore()
    for k in range(1, workers):
        pl.semaphore_signal(
            barrier, inc=1, device_id={"wa": (here + k) % workers}, device_id_type=MESH
        )
    pl.semaphore_wait(barrier, workers - 1)
    copies = []
    for k in range(1, workers):
        to = (here + k) % workers
        copy = pltpu.make_async_remote_copy(
            src_ref=terms.at[pl.ds(pl.multiple_of(to * padded, 8), padded)],
            dst_ref=landed.at[k - 1],
            send_sem=send_sem.at[k - 1],
            recv_sem=recv_sem.at[k - 1],
            device_id={"wa": to},
            device_id_type=MESH,
        )
        copy.start()
        copies.append(copy)
    value = terms[pl.ds(pl.multiple_of(here * padded, 8), padded)]
    for k, copy in enumerate(copies):
        copy.wait_recv()
        value = value + landed[k]
    if len(out.shape) == 1:
        for r in range(out.shape[0] // LANES):
            out[r * LANES : (r + 1) * LANES] = value[r]
    else:
        out[...] = value[: out.shape[0]]
    for copy in copies:
        copy.wait_send()


def body(quartets, counts, eig, freq, phi, cells):
    comps, local_modes = eig.shape
    owners, workers = lax.axis_size("pb"), lax.axis_size("wa")
    held, _, block = quartets.shape
    per_dest = held // workers
    width = math.gcd(local_modes, 1024)
    highs = local_modes // width
    owned = rows_of(comps, highs)
    lanes = math.gcd(local_modes // workers, LANES)
    span = local_modes // workers // lanes
    padded = -(-span // 8) * 8
    vmem = pl.BlockSpec(memory_space=pltpu.VMEM)
    hbm = pl.BlockSpec(memory_space=pltpu.HBM)
    smem = pl.BlockSpec(memory_space=pltpu.SMEM)
    tail = owned - highs * comps
    freq_rows = jnp.pad(freq.reshape(highs, width), ((0, tail - highs), (0, 0)))
    own_deal = quartets.reshape(per_dest, workers, 4, block)
    pieces = 2
    dma = pltpu.SemaphoreType.DMA
    table, pool, tallies = pl.pallas_call(
        functools.partial(gather_kernel, owners, workers, highs),
        out_shape=[
            jax.ShapeDtypeStruct((owners * owned, width), eig.dtype),
            jax.ShapeDtypeStruct((workers, per_dest, 4, block), jnp.int32),
            jax.ShapeDtypeStruct((workers, 1, LANES), jnp.int32),
        ],
        in_specs=[hbm] * 3 + [vmem],
        out_specs=[vmem] * 3,
        scratch_shapes=[dma((highs + 3,))]
        + [dma((owners - 1, pieces))] * 2
        + [dma((owners - 1, pieces, 3))] * 2
        + [dma((workers - 1,))] * 4,
        compiler_params=pltpu.CompilerParams(
            collective_id=0, has_side_effects=True, vmem_limit_bytes=48 << 20
        ),
        name="gather",
    )(eig, freq_rows, own_deal, jnp.full((1, LANES), counts[0], jnp.int32))
    terms = pl.pallas_call(
        functools.partial(rounds_kernel, workers, highs),
        out_shape=jax.ShapeDtypeStruct((workers * padded, LANES), jnp.float32),
        in_specs=[smem] + [vmem] * 4,
        out_specs=vmem,
        scratch_shapes=[pltpu.SMEM((held + 1,), jnp.int32)],
        compiler_params=pltpu.CompilerParams(vmem_limit_bytes=48 << 20),
        name="rounds",
    )(tallies, pool.reshape(held, 4, block), table, phi, cells)
    rates = pl.pallas_call(
        functools.partial(reduce_kernel, workers),
        out_shape=jax.ShapeDtypeStruct(
            (span * LANES,) if lanes == LANES else (span, LANES), jnp.float32
        ),
        in_specs=[vmem],
        out_specs=vmem,
        scratch_shapes=[
            pltpu.VMEM((workers - 1, padded, LANES), jnp.float32),
            dma((workers - 1,)),
            dma((workers - 1,)),
        ],
        compiler_params=pltpu.CompilerParams(
            collective_id=1, has_side_effects=True, vmem_limit_bytes=8 << 20
        ),
        name="reduce",
    )(terms)
    return rates if lanes == LANES else rates[:, :lanes].reshape(span * lanes)


def solution(mesh):
    placed = (P(("pb", "wa"), None, None), P(("pb", "wa")), P(None, "pb"), P("pb"), P(), P())
    return jax.shard_map(
        body, mesh=mesh, in_specs=placed, out_specs=P(("pb", "wa")), check_vma=False
    )
```
